32 devices in a mesh: seq: 8 (over y, x, core), ch: 4 (over z).
Axes of the slice: x: 2, y: 2, z: 4, core: 2. Of those that a mesh axis runs over, the one named last changes fastest.
Arguments:
- inputs: bfloat16 [256, 4096], P('ch', 'seq'), may hold values from -6 to 6
- w_value: bfloat16 [256, 256], P(None, 'ch'), may hold values from -0.375 to 0.375
- w_gate: bfloat16 [256, 256], P(None, 'ch'), may hold values from -0.375 to 0.375
- w_out: bfloat16 [256, 256], P('ch'), may hold values from -0.375 to 0.375
- filter_taps: float32 [256, 4096], P('ch', 'seq'), may hold values from -6 to 6
- grad_out: bfloat16 [256, 4096], P('ch', 'seq'), may hold values from -6 to 6
Outputs:
- d_inputs: bfloat16 [256, 4096], P('ch', 'seq')
- d_w_value: float32 [256, 256], P(None, 'ch')
- d_w_gate: float32 [256, 256], P(None, 'ch')
- d_w_out: float32 [256, 256], P('ch')
- d_filter: float32 [256, 4096], P('ch', 'seq')
The draws below stay inside these ranges and needn't reach their ends.
All inputs are finite; a program needn't handle non-finite values.
Results may differ from the reference program's by a relative error of at most 0.015.
Values may be sent and summed in bfloat16 or wider, within the bound.
A program may use at most 64 MiB of HBM per device.

```python
import math
import jax
import jax.numpy as jnp

D = 256
TOKENS = 4096


def draw_filter_taps(key, part):
    inner_key = jax.random.fold_in(key, 17)
    key_rate, key_jitter = jax.random.split(inner_key)
    upper_log = math.log(3.0 * TOKENS)
    lower_log = math.log(40.0)
    jitter = jax.random.truncated_normal(key_jitter, -6.0, 6.0, (D, TOKENS), jnp.float32)
    timescale = jnp.exp(lower_log + (upper_log - lower_log) * jax.random.uniform(key_rate, (D, 1), jnp.float32))
    decay_rate = 1.0 / timescale
    positions = jnp.arange(TOKENS, dtype=jnp.float32)[None, :]
    normalizer = jnp.sqrt((1.0 - jnp.exp(-2.0 * decay_rate)) / (1.0 - jnp.exp(-2.0 * TOKENS * decay_rate)))
    return (jitter * jnp.exp(-decay_rate * positions) * normalizer).astype(jnp.float32)


def steps_of(stream_key, shape, cuts, low, high):
    gain = 1.0
    for axis_at, parts in cuts:
        steps = jax.random.uniform(jax.random.fold_in(jax.random.fold_in(stream_key, 6), axis_at), (parts,), jnp.float32, low / len(cuts), high / len(cuts))
        gain = gain * jnp.repeat(jnp.exp(steps), shape[axis_at] // parts).reshape((-1,) + (1,) * (len(shape) - 1 - axis_at))
    return gain


def normal_values(stream_key, shape, width, bound, pieces=(), kind=jnp.bfloat16):
    result = width * jax.random.normal(stream_key, shape, jnp.float32)
    if pieces:
        result = result * steps_of(stream_key, shape, pieces, -0.22, 0.18)
    return jnp.clip(result, -bound, bound).astype(kind)


def setup_inputs(seed: int = 0) -> dict:
    seeds = jax.random.split(jax.random.key(seed), 7)
    return {
        "inputs": normal_values(seeds[0], (D, TOKENS), 1.0, 6.0, ((0, 4), (1, 8))),
        "w_value": normal_values(seeds[1], (D, D), D ** -0.5, 0.375, ((1, 4),)),
        "w_gate": normal_values(seeds[2], (D, D), D ** -0.5, 0.375, ((1, 4),)),
        "w_out": normal_values(seeds[3], (D, D), D ** -0.5, 0.375, ((0, 4),)),
        "filter_taps": draw_filter_taps(jax.random.fold_in(seeds[6], 71), 0),
        "grad_out": normal_values(seeds[5], (D, TOKENS), 1.0, 6.0, ((0, 4), (1, 8))),
    }


def reference(inputs, w_value, w_gate, w_out, filter_taps, grad_out):
    padded_len = 2 * TOKENS
    value_proj = jnp.dot(w_value.T, inputs, preferred_element_type=jnp.float32)
    gate_proj = jnp.dot(w_gate.T, inputs, preferred_element_type=jnp.float32)
    spec_filter = jnp.fft.rfft(filter_taps, n=padded_len, axis=1)
    spec_value = jnp.fft.rfft(value_proj, n=padded_len, axis=1)
    mixed_seq = jnp.fft.irfft(spec_filter * spec_value, n=padded_len, axis=1)[:, :TOKENS]
    gated_out = (gate_proj * mixed_seq).astype(jnp.bfloat16)
    d_gated = jnp.dot(w_out, grad_out, preferred_element_type=jnp.float32)
    d_gate = (d_gated * mixed_seq).astype(jnp.bfloat16)
    d_mixed = d_gated * gate_proj
    spec_grad = jnp.fft.rfft(d_mixed, n=padded_len, axis=1)
    d_value = jnp.fft.irfft(jnp.conj(spec_filter) * spec_grad, n=padded_len, axis=1)[:, :TOKENS]
    d_value = d_value.astype(jnp.bfloat16)
    filter_raw = jnp.fft.irfft(jnp.conj(spec_value) * spec_grad, n=padded_len, axis=1)[:, :TOKENS]
    grad_scale = TOKENS ** -0.5
    d_inputs = jnp.dot(w_value, d_value, preferred_element_type=jnp.float32)
    d_inputs = d_inputs + jnp.dot(w_gate, d_gate, preferred_element_type=jnp.float32)
    d_inputs = d_inputs.astype(jnp.bfloat16)
    d_w_value = jnp.dot(inputs, d_value.T, preferred_element_type=jnp.float32) * grad_scale
    d_w_gate = jnp.dot(inputs, d_gate.T, preferred_element_type=jnp.float32) * grad_scale
    d_w_out = jnp.dot(gated_out, grad_out.T, preferred_element_type=jnp.float32) * grad_scale
    d_filter = filter_raw.astype(jnp.float32) * grad_scale
    return d_inputs, d_w_value, d_w_gate, d_w_out, d_filter
```

```python
import functools
import math

import jax
import jax.numpy as jnp
import numpy as np
from jax import lax
from jax.experimental import pallas as pl
from jax.experimental.pallas import tpu as pltpu
from jax.sharding import PartitionSpec as P

F32 = jnp.float32
BF16 = jnp.bfloat16
LANES = 128


def dft_tables(strides, lanes, chans):
    length = 2 * strides * lanes
    n1 = np.arange(strides)
    n2 = np.arange(lanes)
    half = np.arange(strides) + 0.5
    first = np.exp(-2j * np.pi * np.outer(half, n1) / (2 * strides))
    eye = np.eye(chans)
    first_re, first_im = np.kron(first.real, eye), np.kron(first.imag, eye)
    ahead = np.concatenate([first_re, first_im], 0)
    twist = np.repeat(np.exp(-2j * np.pi * np.outer(half, n2) / length), chans, axis=0)
    last = np.exp(-2j * np.pi * np.outer(n2, n2) / lanes)
    c, s = last.real, last.imag
    across = np.block([[c, s], [-s, c]])
    low = lambda a: jnp.asarray(a.astype(np.float32)).astype(BF16)
    wide = lambda a: jnp.asarray(a.astype(np.float32))
    return (
        low(ahead),
        low(ahead.T * (2.0 / length)),
        low(across),
        low(across.T),
        wide(np.stack([twist.real, twist.imag])),
    )


def each(count, step):
    if count <= 16:
        for k in range(count):
            step(k)
    else:
        lax.fori_loop(0, count, lambda k, carry: (step(k), carry)[1], 0)


def body(
    groups, rings, scale,
    in_ref, wv_ref, wg_ref, wo_ref, filt_ref, grad_ref, ahead_ref, back_ref, across_ref, return_ref, twist_ref,
    din_ref, dwv_ref, dwg_ref, dwo_ref, dfil_ref,
    full_in, full_grad, got_filt, out_val, got_val, out_dif, got_dif,
    out_mix, got_mix, out_dv, got_dv, out_df, got_df,
    out_din, got_din, out_w, got_w, out_ws, got_ws,
    seq_send, seq_recv, ch_send, ch_recv,
):
    me = lax.axis_index("seq")
    mc = lax.axis_index("ch")
    ch_rows, tokens = in_ref.shape
    chans = ch_rows // groups
    tiles = tokens // LANES
    width = full_in.shape[0] * ch_rows
    barrier = pltpu.get_barrier_semaphore()

    def seq_peer(k):
        return lax.rem(me + k, groups)

    def seq_from(k):
        return lax.rem(me + groups - k, groups)

    def ch_peer(k):
        return lax.rem(mc + k, rings)

    def ch_from(k):
        return lax.rem(mc + rings - k, rings)

    each(groups - 1, lambda k: pl.semaphore_signal(
        barrier, inc=1, device_id={"seq": seq_peer(k + 1)}, device_id_type=pl.DeviceIdType.MESH))
    each(rings - 1, lambda k: pl.semaphore_signal(
        barrier, inc=1, device_id={"ch": ch_peer(k + 1)}, device_id_type=pl.DeviceIdType.MESH))
    pl.semaphore_wait(barrier, groups + rings - 2)

    def seq_copy(stage, src, dst, k, pick):
        return pltpu.make_async_remote_copy(
            src_ref=src.at[seq_peer(k)] if pick else src,
            dst_ref=dst.at[me],
            send_sem=seq_send.at[stage, k],
            recv_sem=seq_recv.at[stage, k],
            device_id={"seq": seq_peer(k)},
            device_id_type=pl.DeviceIdType.MESH,
        )

    def ch_copy(stage, src, dst, k, pick):
        return pltpu.make_async_remote_copy(
            src_ref=src.at[ch_peer(k)] if pick else src,
            dst_ref=dst.at[mc],
            send_sem=ch_send.at[stage, k],
            recv_sem=ch_recv.at[stage, k],
            device_id={"ch": ch_peer(k)},
            device_id_type=pl.DeviceIdType.MESH,
        )

    def seq_start(stage, src, dst, pick=True):
        each(groups - 1, lambda k: seq_copy(stage, src, dst, k + 1, pick).start())

    def seq_wait(stage, src, dst, pick=True):
        each(groups - 1, lambda k: seq_copy(stage, src, dst, k + 1, pick).wait_recv())

    def seq_done(stage, src, dst, pick=True):
        each(groups - 1, lambda k: seq_copy(stage, src, dst, k + 1, pick).wait_send())

    def ch_start(stage, src, dst, pick=False):
        each(rings - 1, lambda k: ch_copy(stage, src, dst, k + 1, pick).start())

    def ch_wait(stage, src, dst, pick=False):
        each(rings - 1, lambda k: ch_copy(stage, src, dst, k + 1, pick).wait_recv())

    def ch_done(stage, src, dst, pick=False):
        each(rings - 1, lambda k: ch_copy(stage, src, dst, k + 1, pick).wait_send())

    ch_start(0, in_ref, full_in)
    ch_start(1, grad_ref, full_grad)
    seq_start(0, filt_ref, got_filt)
    full_in[mc] = in_ref[...]
    full_grad[mc] = grad_ref[...]
    got_filt[me] = filt_ref[me]

    def by_owner(x):
        x = x.reshape(groups, chans, tokens)
        return jnp.concatenate([x[:, :, j * LANES:(j + 1) * LANES] for j in range(tiles)], axis=1)

    def by_token(x):
        x = x.astype(F32)
        x = jnp.concatenate([x[:, j * chans:(j + 1) * chans, :] for j in range(tiles)], axis=2)
        return x.reshape(ch_rows, tokens)

    def stacked(ref):
        return jnp.concatenate([ref[p] for p in range(groups)], axis=0).astype(BF16)

    ahead = ahead_ref[...]
    across = across_ref[...]
    rows = ahead.shape[1]
    tw_re, tw_im = twist_ref[0], twist_ref[1]

    def dot(a, b):
        return jnp.dot(a, b, preferred_element_type=F32)

    def spectrum(x):
        first = dot(ahead, x)
        re, im = first[:rows], first[rows:]
        mid = jnp.concatenate([re * tw_re - im * tw_im, re * tw_im + im * tw_re], axis=1).astype(BF16)
        out = dot(mid, across)
        return out[:, :LANES], out[:, LANES:]

    def signal(re, im):
        mid = dot(jnp.concatenate([re, im], axis=1).astype(BF16), return_ref[...])
        re, im = mid[:, :LANES], mid[:, LANES:]
        tall = jnp.concatenate([re * tw_re + im * tw_im, im * tw_re - re * tw_im], axis=0).astype(BF16)
        return dot(back_ref[...], tall).reshape(groups, tiles * chans, LANES)

    ch_wait(0, in_ref, full_in)
    x_in = full_in[...].reshape(width, tokens)
    over_first = (((0,), (0,)), ((), ()))
    value = lax.dot_general(wv_ref[...], x_in, over_first, preferred_element_type=F32)
    out_val[...] = by_owner(value).astype(BF16)
    seq_start(1, out_val, got_val)
    got_val[me] = out_val[me]
    gate = lax.dot_general(wg_ref[...], x_in, over_first, preferred_element_type=F32)

    ch_wait(1, grad_ref, full_grad)
    x_grad = full_grad[...].reshape(width, tokens)
    d_gated = dot(wo_ref[...], x_grad)
    out_dif[...] = by_owner(d_gated * gate).astype(BF16)
    seq_start(2, out_dif, got_dif)
    got_dif[me] = out_dif[me]

    seq_wait(0, filt_ref, got_filt)
    by_tile = jnp.concatenate(
        [got_filt[p][:, j * LANES:(j + 1) * LANES] for p in range(groups) for j in range(tiles)], axis=0)
    f_re, f_im = spectrum(by_tile.astype(BF16))
    seq_wait(1, out_val, got_val)
    v_re, v_im = spectrum(stacked(got_val))
    out_mix[...] = signal(f_re * v_re - f_im * v_im, f_re * v_im + f_im * v_re).astype(BF16)
    seq_start(3, out_mix, got_mix)
    got_mix[me] = out_mix[me]

    seq_wait(2, out_dif, got_dif)
    g_re, g_im = spectrum(stacked(got_dif))
    out_dv[...] = signal(f_re * g_re + f_im * g_im, f_re * g_im - f_im * g_re).astype(BF16)
    seq_start(4, out_dv, got_dv)
    got_dv[me] = out_dv[me]
    out_df[...] = signal(v_re * g_re + v_im * g_im, v_re * g_im - v_im * g_re).astype(BF16)
    seq_start(5, out_df, got_df)
    got_df[me] = out_df[me]

    over_last = (((1,), (1,)), ((), ()))
    seq_wait(3, out_mix, got_mix)
    mixed = by_token(got_mix[...])
    gated_out = (gate * mixed).astype(BF16)
    d_gate = (d_gated * mixed).astype(BF16)
    from_gate = dot(wg_ref[...], d_gate)
    out_term = lax.dot_general(gated_out, x_grad, over_last, preferred_element_type=F32)

    seq_wait(4, out_dv, got_dv)
    d_value = by_token(got_dv[...]).astype(BF16)
    d_in = dot(wv_ref[...], d_value) + from_gate
    out_din[...] = d_in.reshape(rings, ch_rows, tokens).astype(BF16)
    ch_start(2, out_din, got_din, True)
    pair_term = lax.dot_general(
        x_in, jnp.concatenate([d_value, d_gate], axis=0), over_last, preferred_element_type=F32)
    pair_rows = width // groups
    pair = pair_term.reshape(groups, pair_rows, 2 * ch_rows)
    outs = out_term.reshape(groups, chans, width)
    out_w[...] = jnp.concatenate(
        [pair] + [outs[:, :, j * LANES:(j + 1) * LANES] for j in range(width // LANES)], axis=1).astype(BF16)
    seq_start(6, out_w, got_w)
    got_w[me] = out_w[me]
    got_din[mc] = out_din[mc]

    seq_wait(6, out_w, got_w)
    total = got_w[0].astype(F32)
    for p in range(1, groups):
        total = total + got_w[p].astype(F32)
    out_ws[...] = total.astype(BF16)
    seq_start(7, out_ws, got_ws, False)
    got_ws[me] = out_ws[...]

    seq_wait(5, out_df, got_df)
    dfil_ref[...] = by_token(got_df[...]) * scale

    ch_wait(2, out_din, got_din, True)
    d_sum = got_din[0].astype(F32)
    for p in range(1, rings):
        d_sum = d_sum + got_din[p].astype(F32)
    din_ref[...] = d_sum.astype(BF16)

    seq_wait(7, out_ws, got_ws, False)
    summed = got_ws[...].astype(F32) * scale
    pair = summed[:, :pair_rows, :].reshape(width, 2 * ch_rows)
    dwv_ref[...] = pair[:, :ch_rows]
    dwg_ref[...] = pair[:, ch_rows:]
    dwo_ref[...] = jnp.concatenate(
        [summed[:, pair_rows + j * chans:pair_rows + (j + 1) * chans, :] for j in range(width // LANES)],
        axis=2).reshape(ch_rows, width)

    ch_done(0, in_ref, full_in)
    ch_done(1, grad_ref, full_grad)
    ch_done(2, out_din, got_din, True)
    for stage, src, dst, pick in (
        (0, filt_ref, got_filt, True), (1, out_val, got_val, True), (2, out_dif, got_dif, True),
        (3, out_mix, got_mix, True), (4, out_dv, got_dv, True), (5, out_df, got_df, True),
        (6, out_w, got_w, True), (7, out_ws, got_ws, False),
    ):
        seq_done(stage, src, dst, pick)


def solution(mesh):
    groups, rings = mesh.shape["seq"], mesh.shape["ch"]

    def on_device(inputs, w_value, w_gate, w_out, filter_taps, grad_out):
        ch_rows, tokens = inputs.shape
        width = w_value.shape[0]
        chans, tiles = ch_rows // groups, tokens // LANES
        tables = dft_tables(groups * tiles, LANES, chans)
        scale = 1.0 / math.sqrt(tokens * groups)
        vmem = pl.BlockSpec(memory_space=pltpu.VMEM)
        block = pltpu.VMEM((groups, tiles * chans, LANES), BF16)
        share = width // groups + chans * (width // LANES)
        return pl.pallas_call(
            functools.partial(body, groups, rings, scale),
            out_shape=(
                jax.ShapeDtypeStruct((ch_rows, tokens), BF16),
                jax.ShapeDtypeStruct((width, ch_rows), F32),
                jax.ShapeDtypeStruct((width, ch_rows), F32),
                jax.ShapeDtypeStruct((ch_rows, width), F32),
                jax.ShapeDtypeStruct((ch_rows, tokens), F32),
            ),
            in_specs=[vmem] * 11,
            out_specs=(vmem,) * 5,
            scratch_shapes=[
                pltpu.VMEM((rings, ch_rows, tokens), BF16),
                pltpu.VMEM((rings, ch_rows, tokens), BF16),
                pltpu.VMEM((groups, chans, tokens), F32),
            ] + [block] * 10 + [
                pltpu.VMEM((rings, ch_rows, tokens), BF16),
                pltpu.VMEM((rings, ch_rows, tokens), BF16),
                pltpu.VMEM((groups, share, 2 * ch_rows), BF16),
                pltpu.VMEM((groups, share, 2 * ch_rows), BF16),
                pltpu.VMEM((share, 2 * ch_rows), BF16),
                pltpu.VMEM((groups, share, 2 * ch_rows), BF16),
                pltpu.SemaphoreType.DMA((8, groups)),
                pltpu.SemaphoreType.DMA((8, groups)),
                pltpu.SemaphoreType.DMA((3, rings)),
                pltpu.SemaphoreType.DMA((3, rings)),
            ],
            compiler_params=pltpu.CompilerParams(collective_id=0, has_side_effects=True),
        )(
            inputs, w_value, w_gate, w_out, filter_taps.reshape(groups, chans, tokens), grad_out, *tables,
        )

    return jax.shard_map(
        on_device,
        mesh=mesh,
        in_specs=(P("ch", "seq"), P(None, "ch"), P(None, "ch"), P("ch", None), P("ch", "seq"), P("ch", "seq")),
        out_specs=(P("ch", "seq"), P(None, "ch"), P(None, "ch"), P("ch", None), P("ch", "seq")),
        check_vma=False,
    )
```

```python
import functools
import math

import jax
import jax.numpy as jnp
import numpy as np
from jax import lax
from jax.experimental import pallas as pl
from jax.experimental.pallas import tpu as pltpu
from jax.sharding import PartitionSpec as P

F32 = jnp.float32
BF16 = jnp.bfloat16
LANES = 128


def dft_tables(strides, lanes, chans):
    length = 2 * strides * lanes
    n1 = np.arange(strides)
    n2 = np.arange(lanes)
    half = np.arange(strides) + 0.5
    first = np.exp(-2j * np.pi * np.outer(half, n1) / (2 * strides))
    eye = np.eye(chans)
    first_re, first_im = np.kron(first.real, eye), np.kron(first.imag, eye)
    ahead = np.concatenate([first_re, first_im], 0)
    twist = np.repeat(np.exp(-2j * np.pi * np.outer(half, n2) / length), chans, axis=0)
    last = np.exp(-2j * np.pi * np.outer(n2, n2) / lanes)
    c, s = last.real, last.imag
    across = np.block([[c, s], [-s, c]])
    low = lambda a: jnp.asarray(a.astype(np.float32)).astype(BF16)
    wide = lambda a: jnp.asarray(a.astype(np.float32))
    return (
        low(ahead),
        low(ahead.T * (2.0 / length)),
        low(across),
        low(across.T),
        wide(np.stack([twist.real, twist.imag])),
    )


def each(count, step):
    if count <= 16:
        for k in range(count):
            step(k)
    else:
        lax.fori_loop(0, count, lambda k, carry: (step(k), carry)[1], 0)


def body(
    groups, rings,
    in_ref, wv_ref, wg_ref, wo_ref, filt_ref, grad_ref, ahead_hbm, back_hbm, across_hbm, return_hbm, twist_hbm,
    din_ref, dw_ref, dfil_ref,
    full_in, full_grad, got_filt, out_val, got_val, out_dif, got_dif,
    out_mix, got_mix, out_dv, got_dv, out_df, got_df,
    out_din, got_din, out_w, got_w, out_ws, got_ws, out_v, got_v, out_vs, got_vs,
    ahead_ref, back_ref, across_ref, return_ref, twist_ref,
    seq_send, seq_recv, ch_send, ch_recv, line_send, line_recv, table_sem,
):
    me = lax.axis_index("seq")
    mc = lax.axis_index("ch")
    ch_rows, tokens = in_ref.shape
    chans = ch_rows // groups
    tiles = tokens // LANES
    width = full_in.shape[0] * ch_rows
    barrier = pltpu.get_barrier_semaphore()

    def seq_peer(k):
        return lax.rem(me + k, groups)

    def ch_peer(k):
        return lax.rem(mc + k, rings)

    each(groups - 1, lambda k: pl.semaphore_signal(
        barrier, inc=1, device_id={"seq": seq_peer(k + 1)}, device_id_type=pl.DeviceIdType.MESH))
    each(rings - 1, lambda k: pl.semaphore_signal(
        barrier, inc=1, device_id={"ch": ch_peer(k + 1)}, device_id_type=pl.DeviceIdType.MESH))
    tables = [
        pltpu.make_async_copy(src, dst, table_sem.at[i])
        for i, (src, dst) in enumerate((
            (ahead_hbm, ahead_ref), (twist_hbm, twist_ref), (across_hbm, across_ref),
            (return_hbm, return_ref), (back_hbm, back_ref)))
    ]
    for table in tables:
        table.start()
    pl.semaphore_wait(barrier, groups + rings - 2)

    def seq_copy(stage, src, dst, k, pick):
        return pltpu.make_async_remote_copy(
            src_ref=src.at[seq_peer(k)] if pick else src,
            dst_ref=dst.at[me],
            send_sem=seq_send.at[stage, k],
            recv_sem=seq_recv.at[stage, k],
            device_id={"seq": seq_peer(k)},
            device_id_type=pl.DeviceIdType.MESH,
        )

    def ch_copy(src, dst, k):
        return pltpu.make_async_remote_copy(
            src_ref=src.at[ch_peer(k)],
            dst_ref=dst.at[mc],
            send_sem=ch_send.at[k],
            recv_sem=ch_recv.at[k],
            device_id={"ch": ch_peer(k)},
            device_id_type=pl.DeviceIdType.MESH,
        )

    def seq_start(stage, src, dst, pick=True):
        each(groups - 1, lambda k: seq_copy(stage, src, dst, k + 1, pick).start())

    def seq_wait(stage, src, dst, pick=True):
        each(groups - 1, lambda k: seq_copy(stage, src, dst, k + 1, pick).wait_recv())

    def seq_done(stage, src, dst, pick=True):
        each(groups - 1, lambda k: seq_copy(stage, src, dst, k + 1, pick).wait_send())

    wholes = (full_in, full_grad)
    owns = (in_ref, grad_ref)

    def hop(array, block, step, own):
        return pltpu.make_async_remote_copy(
            src_ref=owns[array] if own else wholes[array].at[block],
            dst_ref=wholes[array].at[block],
            send_sem=line_send.at[array, (step + 1) // 2, block],
            recv_sem=line_recv.at[array, block],
            device_id={"ch": mc + step},
            device_id_type=pl.DeviceIdType.MESH,
        )

    def can(step):
        return mc < rings - 1 if step == 1 else mc > 0

    def present(step, far):
        return mc >= far if step == 1 else mc < rings - far

    def line_open(array):
        for step in (1, -1):
            @pl.when(can(step))
            def _():
                hop(array, mc, step, True).start()

    def line_take(array, far):
        for step in (1, -1):
            @pl.when(present(step, far))
            def _():
                hop(array, mc - step * far, step, False).wait_recv()
                if far < rings - 1:
                    @pl.when(can(step))
                    def _():
                        hop(array, mc - step * far, step, False).start()

    def line_close(array):
        for step in (1, -1):
            @pl.when(can(step))
            def _():
                hop(array, mc, step, True).wait_send()
                for far in range(1, rings - 1):
                    @pl.when(present(step, far))
                    def _():
                        hop(array, mc - step * far, step, False).wait_send()

    line_open(0)
    line_open(1)
    seq_start(0, filt_ref, got_filt)
    full_in[mc] = in_ref[...]
    full_grad[mc] = grad_ref[...]
    got_filt[me] = filt_ref[me]

    def by_owner(x):
        x = x.reshape(groups, chans, tokens)
        return jnp.concatenate([x[:, :, j * LANES:(j + 1) * LANES] for j in range(tiles)], axis=1)

    def by_token(x):
        x = x.astype(F32)
        x = jnp.concatenate([x[:, j * chans:(j + 1) * chans, :] for j in range(tiles)], axis=2)
        return x.reshape(ch_rows, tokens)

    def stacked(ref):
        return jnp.concatenate([ref[p] for p in range(groups)], axis=0).astype(BF16)

    rows = ahead_ref.shape[1]

    def dot(a, b):
        return jnp.dot(a, b, preferred_element_type=F32)

    def spectrum(x):
        first = dot(ahead_ref[...], x)
        re, im = first[:rows], first[rows:]
        tw_re, tw_im = twist_ref[0], twist_ref[1]
        mid = jnp.concatenate([re * tw_re - im * tw_im, re * tw_im + im * tw_re], axis=1).astype(BF16)
        out = dot(mid, across_ref[...])
        return out[:, :LANES], out[:, LANES:]

    def signal(re, im):
        mid = dot(jnp.concatenate([re, im], axis=1).astype(BF16), return_ref[...])
        re, im = mid[:, :LANES], mid[:, LANES:]
        tw_re, tw_im = twist_ref[0], twist_ref[1]
        tall = jnp.concatenate([re * tw_re + im * tw_im, im * tw_re - re * tw_im], axis=0).astype(BF16)
        return dot(back_ref[...], tall).reshape(groups, tiles * chans, LANES)

    over_first = (((0,), (0,)), ((), ()))
    over_last = (((1,), (1,)), ((), ()))
    for far in range(1, rings - 1):
        line_take(0, far)
        line_take(1, far)

    for table in tables:
        table.wait()
    seq_wait(0, filt_ref, got_filt)
    by_tile = jnp.concatenate(
        [got_filt[p][:, j * LANES:(j + 1) * LANES] for p in range(groups) for j in range(tiles)], axis=0)
    f_re, f_im = spectrum(by_tile.astype(BF16))

    line_take(0, rings - 1)
    x_in = full_in[...].reshape(width, tokens)
    value = dot(wv_ref[...], x_in)
    out_val[...] = by_owner(value).astype(BF16)
    seq_start(1, out_val, got_val)
    got_val[me] = out_val[me]
    gate = dot(wg_ref[...], x_in)

    line_take(1, rings - 1)
    x_grad = full_grad[...].reshape(width, tokens)
    d_gated = dot(wo_ref[...], x_grad)
    out_dif[...] = by_owner(d_gated * gate).astype(BF16)
    seq_start(2, out_dif, got_dif)
    got_dif[me] = out_dif[me]

    seq_wait(1, out_val, got_val)
    v_re, v_im = spectrum(stacked(got_val))
    out_mix[...] = signal(f_re * v_re - f_im * v_im, f_re * v_im + f_im * v_re).astype(BF16)
    seq_start(3, out_mix, got_mix)
    got_mix[me] = out_mix[me]

    seq_wait(2, out_dif, got_dif)
    g_re, g_im = spectrum(stacked(got_dif))
    out_dv[...] = signal(f_re * g_re + f_im * g_im, f_re * g_im - f_im * g_re).astype(BF16)
    seq_start(4, out_dv, got_dv)
    got_dv[me] = out_dv[me]
    out_df[...] = signal(v_re * g_re + v_im * g_im, v_re * g_im - v_im * g_re).astype(BF16)
    seq_start(5, out_df, got_df)
    got_df[me] = out_df[me]

    parts = width // LANES

    def by_share(x):
        x = x.reshape(groups, chans, width)
        return jnp.concatenate([x[:, :, j * LANES:(j + 1) * LANES] for j in range(parts)], axis=1)

    def by_width(x):
        return jnp.concatenate([x[:, j * chans:(j + 1) * chans, :] for j in range(parts)], axis=2).reshape(ch_rows, width)

    def total(ref):
        out = ref[0].astype(F32)
        for p in range(1, ref.shape[0]):
            out = out + ref[p].astype(F32)
        return out.astype(BF16)

    seq_wait(3, out_mix, got_mix)
    mixed = by_token(got_mix[...])
    gated_out = (gate * mixed).astype(BF16)
    d_gate = (d_gated * mixed).astype(BF16)
    gate_term = lax.dot_general(d_gate, x_in, over_last, preferred_element_type=F32)
    out_term = lax.dot_general(gated_out, x_grad, over_last, preferred_element_type=F32)
    out_w[...] = jnp.concatenate([by_share(gate_term), by_share(out_term)], axis=1).astype(BF16)
    seq_start(6, out_w, got_w)
    got_w[me] = out_w[me]
    from_gate = lax.dot_general(wg_ref[...], d_gate, over_first, preferred_element_type=F32)

    seq_wait(4, out_dv, got_dv)
    d_value = by_token(got_dv[...]).astype(BF16)
    d_in = lax.dot_general(wv_ref[...], d_value, over_first, preferred_element_type=F32) + from_gate
    out_din[...] = d_in.reshape(rings, ch_rows, tokens).astype(BF16)
    each(rings - 1, lambda k: ch_copy(out_din, got_din, k + 1).start())
    value_term = lax.dot_general(d_value, x_in, over_last, preferred_element_type=F32)
    out_v[...] = by_share(value_term).astype(BF16)
    seq_start(8, out_v, got_v)
    got_v[me] = out_v[me]
    got_din[mc] = out_din[mc]

    seq_wait(6, out_w, got_w)
    out_ws[...] = total(got_w)
    seq_start(7, out_ws, got_ws, False)
    got_ws[me] = out_ws[...]

    seq_wait(5, out_df, got_df)
    dfil_ref[...] = by_token(got_df[...])

    seq_wait(8, out_v, got_v)
    out_vs[...] = total(got_v)
    seq_start(9, out_vs, got_vs, False)
    got_vs[me] = out_vs[...]

    seq_wait(7, out_ws, got_ws, False)
    half = parts * chans
    summed = got_ws[...].astype(F32)
    dw_ref[1] = by_width(summed[:, :half, :])
    dw_ref[2] = by_width(summed[:, half:, :])
    each(rings - 1, lambda k: ch_copy(out_din, got_din, k + 1).wait_recv())
    din_ref[...] = total(got_din)
    seq_wait(9, out_vs, got_vs, False)
    dw_ref[0] = by_width(got_vs[...].astype(F32))

    line_close(0)
    line_close(1)
    each(rings - 1, lambda k: ch_copy(out_din, got_din, k + 1).wait_send())
    for stage, src, dst, pick in (
        (0, filt_ref, got_filt, True), (1, out_val, got_val, True), (2, out_dif, got_dif, True),
        (3, out_mix, got_mix, True), (4, out_dv, got_dv, True), (5, out_df, got_df, True),
        (6, out_w, got_w, True), (7, out_ws, got_ws, False), (8, out_v, got_v, True), (9, out_vs, got_vs, False),
    ):
        seq_done(stage, src, dst, pick)


def finish(scale, din_ref, dw_ref, dfil_ref, din_out, dwv_out, dwg_out, dwo_out, dfil_out):
    din_out[...] = din_ref[...]
    dwv_out[...] = dw_ref[0] * scale
    dwg_out[...] = dw_ref[1] * scale
    dwo_out[...] = dw_ref[2] * scale
    dfil_out[...] = dfil_ref[...] * scale


def solution(mesh):
    groups, rings = mesh.shape["seq"], mesh.shape["ch"]

    def on_device(inputs, w_value, w_gate, w_out, filter_taps, grad_out):
        ch_rows, tokens = inputs.shape
        width = w_value.shape[0]
        chans, tiles, parts = ch_rows // groups, tokens // LANES, width // LANES
        tables = dft_tables(groups * tiles, LANES, chans)
        scale = 1.0 / math.sqrt(tokens * groups)
        vmem = pl.BlockSpec(memory_space=pltpu.VMEM)
        hbm = pl.BlockSpec(memory_space=pl.ANY)
        block = pltpu.VMEM((groups, tiles * chans, LANES), BF16)
        whole = pltpu.VMEM((rings, ch_rows, tokens), BF16)
        share = lambda count: [
            pltpu.VMEM((groups, count * parts * chans, LANES), BF16),
            pltpu.VMEM((groups, count * parts * chans, LANES), BF16),
            pltpu.VMEM((count * parts * chans, LANES), BF16),
            pltpu.VMEM((groups, count * parts * chans, LANES), BF16),
        ]
        tokens_out = jax.ShapeDtypeStruct((ch_rows, tokens), F32)
        weight_out = jax.ShapeDtypeStruct((ch_rows, width), F32)
        d_inputs, d_weights, d_filter = pl.pallas_call(
            functools.partial(body, groups, rings),
            out_shape=(
                jax.ShapeDtypeStruct((ch_rows, tokens), BF16),
                jax.ShapeDtypeStruct((3, ch_rows, width), F32),
                tokens_out,
            ),
            in_specs=[vmem] * 6 + [hbm] * 5,
            out_specs=(vmem,) * 3,
            scratch_shapes=[whole, whole, pltpu.VMEM((groups, chans, tokens), F32)] + [block] * 10
            + [whole, whole] + share(2) + share(1)
            + [pltpu.VMEM(table.shape, table.dtype) for table in tables] + [
                pltpu.SemaphoreType.DMA((10, groups)),
                pltpu.SemaphoreType.DMA((10, groups)),
                pltpu.SemaphoreType.DMA((rings,)),
                pltpu.SemaphoreType.DMA((rings,)),
                pltpu.SemaphoreType.DMA((2, 2, rings)),
                pltpu.SemaphoreType.DMA((2, rings)),
                pltpu.SemaphoreType.DMA((5,)),
            ],
            compiler_params=pltpu.CompilerParams(collective_id=0, has_side_effects=True),
        )(
            inputs, w_value.T, w_gate.T, w_out, filter_taps.reshape(groups, chans, tokens), grad_out, *tables,
        )
        d_inputs, d_w_value, d_w_gate, d_w_out, d_filter = pl.pallas_call(
            functools.partial(finish, scale),
            out_shape=(
                jax.ShapeDtypeStruct((ch_rows, tokens), BF16), weight_out, weight_out, weight_out, tokens_out,
            ),
            in_specs=[vmem] * 3,
            out_specs=(vmem,) * 5,
        )(d_inputs, d_weights, d_filter)
        return d_inputs, d_w_value.T, d_w_gate.T, d_w_out, d_filter

    return jax.shard_map(
        on_device,
        mesh=mesh,
        in_specs=(P("ch", "seq"), P(None, "ch"), P(None, "ch"), P("ch", None), P("ch", "seq"), P("ch", "seq")),
        out_specs=(P("ch", "seq"), P(None, "ch"), P(None, "ch"), P("ch", None), P("ch", "seq")),
        check_vma=False,
    )
```
